32 devices in a mesh: band: 16 (over z, x, core), ga: 2 (over y).
Axes of the slice: x: 2, y: 2, z: 4, core: 2. Of those that a mesh axis runs over, the one named last changes fastest.
Arguments:
- psi: float32 [2, 4096, 65536], P(None, 'band', 'ga'), may hold values from -0.0234375 to 0.0234375
- hx: float32 [2, 256, 65536], P(None, 'band', 'ga'), may hold values from -6 to 6
Outputs:
- h_sub: float32 [2, 4096, 256], P(None, ('band', 'ga'))
The draws below stay inside these ranges and needn't reach their ends.
All inputs are finite; a program needn't handle non-finite values.
Results may differ from the reference program's by a relative error of at most 0.00007.
Values sent between devices are 32-bit elements; how exact they have to be, the bound alone decides.
No kernel may reach another device: no remote copies, remote signals or barrier semaphores. Data moves between devices by JAX's collectives and lax.ppermute only.
A program may use at most 192 MiB of HBM per device.

```python
import jax
import jax.numpy as jnp
from jax import lax

NB = 4096
NG = 65536
NBLK = 256


def level_of(stream_key, dims, shards, smallest, high):
    def one(position, shards_of):
        draws = jax.random.uniform(jax.random.fold_in(jax.random.fold_in(stream_key, 6), position), (shards_of,), jnp.float32, smallest / len(shards), high / len(shards))
        return jnp.repeat(jnp.exp(draws), dims[position] // shards_of).reshape((-1,) + (1,) * (len(dims) - position - 1))

    gain = one(*shards[0])
    for cut in shards[1:]:
        gain = gain * one(*cut)
    return gain


def gaussian(key, extent, scale, reach, split=(), held_as=jnp.bfloat16):
    factor_of = level_of(key, extent, split, -0.22, 0.18) if split else 1.0
    entries = jax.random.normal(key, extent, jnp.float32) * scale * factor_of
    return jnp.minimum(jnp.maximum(entries, -reach), reach).astype(held_as)


def setup_inputs(seed: int = 0) -> dict:
    key_list = jax.random.split(jax.random.key(seed), 3)
    psi = gaussian(key_list[0], (2, NB, NG), NG ** -0.5, 0.0234375, ((1, 16), (2, 2)), jnp.float32)
    hx = gaussian(key_list[1], (2, NBLK, NG), 1.0, 6.0, ((1, 16), (2, 2)), jnp.float32)
    return dict(psi=psi, hx=hx)


def contract(left, right):
    return lax.dot_general(left, right, (((1,), (1,)), ((), ())), precision=lax.Precision.HIGHEST, preferred_element_type=jnp.float32)


def reference(psi, hx):
    real_part = contract(psi[0], hx[0]) + contract(psi[1], hx[1])
    imag_part = contract(psi[0], hx[1]) - contract(psi[1], hx[0])
    return jnp.stack([real_part, imag_part], axis=0)
```

```python
import functools

import jax
import jax.numpy as jnp
from jax import lax
from jax.experimental import pallas as pl
from jax.experimental.pallas import tpu as pltpu
from jax.sharding import PartitionSpec as P


F32, BF16 = jnp.float32, jnp.bfloat16
PIECES = (3, 3, 3, 3, 3, 3, 3, 3, 3, 3, 2)
STEP = 1024


def chip_ring(mesh):
    devices = mesh.devices[:, 0]
    if len(devices) % 2:
        return None
    at = [getattr(d, "coords", None) for d in devices]
    if any(c is None for c in at) or any(at[2 * m] != at[2 * m + 1] for m in range(len(at) // 2)):
        return list(range(len(at) // 2))
    at = [tuple(c) for c in at[::2]]
    n = len(at)
    near = [
        [b for b in range(n) if sum(abs(i - j) for i, j in zip(at[a], at[b])) == 1]
        for a in range(n)
    ]

    def extend(path):
        if len(path) == n:
            return path if n <= 2 or path[0] in near[path[-1]] else None
        for b in near[path[-1]]:
            if b not in path:
                found = extend(path + [b])
                if found:
                    return found
        return None

    return extend([0]) or list(range(n))


def product(kinds, ends, first, last, table, psi, own, *refs):
    moved = len(kinds) - 1
    rest = refs[moved * len(ends) :]
    if not first:
        acc_in, rest = rest[0], rest[1:]
    if last:
        keep, send, acc, xh, xl, ph, lo_p = rest
    else:
        out, acc, xh, xl, ph, lo_p = rest
    step = pl.program_id(0)
    bands, rows = ph.shape[0] // 2, xh.shape[0] // 2
    band = lax.axis_index("band")
    base = band * len(kinds)

    @pl.when(step == 0)
    def _():
        for part in range(2):
            at = slice(part * bands, (part + 1) * bands)
            acc[at, :] = jnp.zeros((bands, 2 * rows), F32) if first else acc_in[part]

    def put(part, i, x):
        at = pl.multiple_of(table[base + i] + part * rows, 16)
        hi = x.astype(BF16)
        xh[pl.ds(at, x.shape[0]), :] = hi
        xl[pl.ds(at, x.shape[0]), :] = (x - hi.astype(F32)).astype(BF16)

    def put_all(xs, kinds, skip):
        for i, (ref, kind) in enumerate(zip(xs, kinds), skip):
            if kind == "block":
                put(0, i, ref[0])
                put(1, i, ref[1])
            elif kind == "far":
                put(band % 2, i, ref[0])
            else:
                put(1 - band % 2, i, ref[0])

    put_all((own,), kinds[:1], 0)
    for j, end in enumerate(ends):
        xs = refs[j * moved : (j + 1) * moved]
        if len(ends) == 1:
            put_all(xs, kinds[1:], 1)
        else:
            began = ends[j - 1] if j else 0
            pl.when((step >= began) & (step < end))(functools.partial(put_all, xs, kinds[1:], 1))
    for part in range(2):
        x = psi[part]
        hi = x.astype(BF16)
        ph[part * bands : (part + 1) * bands, :] = hi
        lo_p[part * bands : (part + 1) * bands, :] = (x - hi.astype(F32)).astype(BF16)

    def dot(a, b):
        return lax.dot_general(a[...], b[...], (((1,), (1,)), ((), ())), preferred_element_type=F32)

    acc[...] += dot(ph, xl) + dot(lo_p, xh) + dot(ph, xh)

    @pl.when(step == pl.num_programs(0) - 1)
    def _():
        if last:
            half = keep.shape[1]
            ga = lax.axis_index("ga")
            for ref, at in ((keep, ga * half), (send, (1 - ga) * half)):
                above = pl.ds(pl.multiple_of(at, half), half)
                below = pl.ds(pl.multiple_of(at + bands, half), half)
                ref[0] = acc[above, :rows] + acc[below, rows:]
                ref[1] = acc[above, rows:] - acc[below, :rows]
        else:
            out[0] = acc[:bands, :]
            out[1] = acc[bands:, :]


def add_pieces(table, kinds, psi, hx, blocks, vectors, acc, start, sizes, last=False):
    size = sum(sizes)
    bands = psi.shape[1]
    step = max(d for d in (STEP, 512, 256, 128) if all(n % d == 0 for n in (start, *sizes)))
    at = start // step
    ends = [sum(sizes[: j + 1]) // step for j in range(len(sizes))]

    specs = [
        pl.BlockSpec((2, bands, step), lambda k, s: (0, 0, at + k)),
        pl.BlockSpec((2, hx.shape[1], step), lambda k, s: (0, 0, at + k)),
    ]
    operands = [psi, hx]
    for j, end in enumerate(ends):
        began = ends[j - 1] if j else 0

        def piece(k, s, began=began, end=end):
            return (0, 0, jnp.clip(k - began, 0, end - began - 1) if len(ends) > 1 else k)

        for b in blocks[j]:
            specs.append(pl.BlockSpec((b.shape[0], b.shape[1], step), piece))
            operands.append(b)
    if acc is not None:
        specs.append(pl.BlockSpec((2, bands, 2 * vectors), lambda k, s: (0, 0, 0)))
        operands.append(acc)
    shape = (2, bands // 2, vectors) if last else (2, bands, 2 * vectors)
    out_shape = jax.ShapeDtypeStruct(shape, F32)
    out_spec = pl.BlockSpec(shape, lambda k, s: (0, 0, 0))
    return pl.pallas_call(
        functools.partial(product, kinds, ends, acc is None, last),
        out_shape=(out_shape, out_shape) if last else out_shape,
        grid_spec=pltpu.PrefetchScalarGridSpec(
            num_scalar_prefetch=1,
            grid=(size // step,),
            in_specs=specs,
            out_specs=(out_spec, out_spec) if last else out_spec,
            scratch_shapes=[
                pltpu.VMEM((2 * bands, 2 * vectors), F32),
                pltpu.VMEM((2 * vectors, step), BF16),
                pltpu.VMEM((2 * vectors, step), BF16),
                pltpu.VMEM((2 * bands, step), BF16),
                pltpu.VMEM((2 * bands, step), BF16),
            ],
        ),
        compiler_params=pltpu.CompilerParams(vmem_limit_bytes=20 << 20),
        cost_estimate=pl.CostEstimate(
            flops=3 * 8 * bands * vectors * size,
            bytes_accessed=8 * (bands + vectors) * size,
            transcendentals=0,
        ),
    )(table, *operands)


def solution(mesh):
    n_band, n_ga = mesh.shape["band"], mesh.shape["ga"]
    ring = chip_ring(mesh)
    chips = len(ring)
    place = [0] * chips
    for r, m in enumerate(ring):
        place[m] = r
    onward = [(2 * m + c, 2 * ring[(place[m] + (1 if c == 0 else -1)) % chips] + c) for m in range(chips) for c in (0, 1)]
    across = [(b, b ^ 1) for b in range(n_band)]
    full = (chips - 1) // 2
    half = chips % 2 == 0
    hops = full + half

    def hop(x):
        return lax.ppermute(x, "band", onward)

    def swap(x):
        return lax.ppermute(x, "band", across)

    def per_device(psi, hx):
        v, g = hx.shape[1], hx.shape[2]
        band = lax.axis_index("band")
        core = band % 2
        kinds = ["block"] * (2 + 2 * full) + (["far", "near"] if half else [])
        table = []
        for b in range(n_band):
            m, c = b // 2, b % 2
            way = 1 if c else -1
            at = [2 * m + c, 2 * m + 1 - c]
            for s in range(1, full + 1):
                at += [2 * ring[(place[m] + d) % chips] for d in (s * way, -s * way)]
            if half:
                at += [2 * ring[(place[m] + full + 1) % chips]] * 2
            table += [v * i for i in at]
        table = jnp.array(table, jnp.int32)

        unit = g // sum(PIECES)
        starts = [unit * sum(PIECES[:i]) for i in range(len(PIECES))]
        blocks = {}

        def chip_block(i):
            own = lax.slice_in_dim(hx, starts[i], starts[i] + PIECES[i] * unit, axis=2)
            other = swap(own)
            low, high = jnp.where(core == 0, own, other), jnp.where(core == 0, other, own)
            blocks[i] = [other]
            return jnp.concatenate([low, high], axis=1)

        def travel(i, s, x):
            if s > full:
                x = jnp.where(core == 0, x[0:1], x[1:2])
            x = hop(x)
            y = swap(x)
            blocks[i] += [x, y]
            return x

        acc = None
        final = len(PIECES) - 1
        for i in range(len(PIECES)):
            x = chip_block(i)
            for s in range(1, hops + 1):
                x = travel(i, s, x)
            last = i == final and n_ga == 2
            acc = add_pieces(table, kinds, psi, hx, [blocks[i]], n_band * v, acc, starts[i], [PIECES[i] * unit], last)
        if n_ga != 2:
            both = n_band * v
            acc = jnp.stack([acc[0, :, :both] + acc[1, :, both:], acc[0, :, both:] - acc[1, :, :both]])
            return lax.psum_scatter(acc, "ga", scatter_dimension=1, tiled=True)

        keep, send = acc
        return keep + lax.ppermute(send, "ga", [(0, 1), (1, 0)])

    spec = P(None, "band", "ga")
    return jax.shard_map(
        per_device,
        mesh=mesh,
        in_specs=(spec, spec),
        out_specs=P(None, ("band", "ga"), None),
        check_vma=False,
    )
```
